32 devices in a mesh: seq: 4 (over y, x), fsdp: 8 (over z, core).
Axes of the slice: x: 2, y: 2, z: 4, core: 2. Of those that a mesh axis runs over, the one named last changes fastest.
Arguments:
- tokens: bfloat16 [8, 512, 8192], P('fsdp', 'seq'), may hold values from -6 to 6
- norm_gain: float32 [8192], replicated, may hold values from 0.3 to 3
- w_query: bfloat16 [8192, 4096], P(('seq', 'fsdp')), may hold values from -1 to 1
- key_weight: bfloat16 [8192, 512], P(('seq', 'fsdp')), may hold values from -1 to 1
- value_weight: bfloat16 [8192, 512], P(('seq', 'fsdp')), may hold values from -0.0625 to 0.0625
- w_out: bfloat16 [4096, 8192], P(None, ('seq', 'fsdp')), may hold values from -0.09375 to 0.09375
Outputs:
- result: float32 [8, 512, 8192], P('fsdp', 'seq')
The draws below stay inside these ranges and needn't reach their ends.
All inputs are finite; a program needn't handle non-finite values.
Results may differ from the reference program's by a relative error of at most 0.04.
Values may be sent and summed in bfloat16 or wider, within the bound.
No kernel may reach another device: no remote copies, remote signals or barrier semaphores. Data moves between devices by JAX's collectives and lax.ppermute only.
A program may use at most 128 MiB of HBM per device.

```python
import math
import jax
import jax.numpy as jnp
from jax import lax

MODEL_WIDTH = 8192
HQ = 32
KEY_VALUE_HEADS = 4
HEAD_SIZE = 128
GROUP = 8
SEQUENCE_TOKENS = 512
SEQS = 8
N_SEQ = 4


def projection_sample(key, head_count):
    normal_draw = jax.random.normal(jax.random.fold_in(key, 11), (MODEL_WIDTH, head_count * HEAD_SIZE), jnp.float32)
    normal_draw = jnp.clip(normal_draw, -6.0, 6.0) / math.sqrt(MODEL_WIDTH)
    normal_draw = jnp.clip(normal_draw, -1.0, 1.0)
    return normal_draw.astype(jnp.bfloat16)


def draw_w_query(key, part):
    return projection_sample(jax.random.fold_in(key, 101), HQ)


def draw_key_weight(key, part):
    return projection_sample(jax.random.fold_in(key, 202), KEY_VALUE_HEADS)


def shard_levels(rng, extent, split, smallest, top_value):
    def one(position, parts):
        heights = jax.random.uniform(jax.random.fold_in(jax.random.fold_in(rng, 6), position), (parts,), jnp.float32, smallest / len(split), top_value / len(split))
        return jnp.repeat(jnp.exp(heights), extent[position] // parts).reshape((-1,) + (1,) * (len(extent) - position - 1))

    level = one(*split[0])
    for cut in split[1:]:
        level = level * one(*cut)
    return level


def bell_draw(own_key, extent, deviation, bound, shards=(), kind=jnp.bfloat16):
    entries = jax.random.normal(own_key, extent, jnp.float32) * deviation
    if len(shards) > 0:
        entries = shard_levels(own_key, extent, shards, -0.22, 0.18) * entries
    return jnp.clip(entries, min=-bound, max=bound).astype(kind)


def setup_inputs(seed: int = 0) -> dict:
    splits = jax.random.split(jax.random.key(seed), 7)
    tokens = bell_draw(splits[0], (SEQS, SEQUENCE_TOKENS, MODEL_WIDTH), 1.0, 6.0, ((0, 8), (1, 4)))
    norm_gain = jnp.clip(jnp.exp(jax.random.uniform(splits[1], (MODEL_WIDTH,), jnp.float32, math.log(0.3), math.log(3.0))), 0.3, 3.0)
    w_query = draw_w_query(jax.random.fold_in(splits[6], 71), 0)
    key_weight = draw_key_weight(jax.random.fold_in(splits[6], 71), 0)
    value_weight = bell_draw(splits[4], (MODEL_WIDTH, KEY_VALUE_HEADS * HEAD_SIZE), MODEL_WIDTH ** -0.5, 0.0625, ((0, 32),))
    w_out = bell_draw(splits[5], (HQ * HEAD_SIZE, MODEL_WIDTH), (HQ * HEAD_SIZE) ** -0.5, 0.09375, ((1, 32),))
    return {"tokens": tokens, "norm_gain": norm_gain, "w_query": w_query, "key_weight": key_weight, "value_weight": value_weight, "w_out": w_out}


def rms_norm(sequence_rows, norm_gain):
    floats = sequence_rows.astype(jnp.float32)
    mean_square = lax.optimization_barrier(jnp.mean(floats * floats, axis=-1, keepdims=True))
    return (floats * lax.rsqrt(mean_square + 1e-05) * norm_gain).astype(jnp.bfloat16)

def apply_projection(normed_input, weight):
    block = MODEL_WIDTH // N_SEQ
    running = jnp.zeros((normed_input.shape[0], weight.shape[1]), jnp.float32)
    for block_index in range(N_SEQ):
        partial_sum = jnp.dot(normed_input[:, block_index * block:(block_index + 1) * block], weight[block_index * block:(block_index + 1) * block], preferred_element_type=jnp.float32)
        rounded = lax.optimization_barrier(partial_sum.astype(jnp.bfloat16))
        running = running + rounded.astype(jnp.float32)
    return running.astype(jnp.bfloat16)

def reference(tokens, norm_gain, w_query, key_weight, value_weight, w_out):
    scale = HEAD_SIZE ** (-0.5)
    row_ids = lax.broadcasted_iota(jnp.int32, (SEQUENCE_TOKENS, SEQUENCE_TOKENS), 0)
    col_ids = lax.broadcasted_iota(jnp.int32, (SEQUENCE_TOKENS, SEQUENCE_TOKENS), 1)
    causal = row_ids >= col_ids

    def one_sequence(sequence_rows):
        normed_input = rms_norm(sequence_rows, norm_gain)
        queries = apply_projection(normed_input, w_query).reshape(SEQUENCE_TOKENS, HQ, HEAD_SIZE)
        key_tensor = apply_projection(normed_input, key_weight).reshape(SEQUENCE_TOKENS, KEY_VALUE_HEADS, HEAD_SIZE)
        value_tensor = apply_projection(normed_input, value_weight).reshape(SEQUENCE_TOKENS, KEY_VALUE_HEADS, HEAD_SIZE)

        def one_head(head_index):
            query_head = lax.dynamic_index_in_dim(queries, head_index, 1, keepdims=False)
            kv_index = head_index // GROUP
            key_head = lax.dynamic_index_in_dim(key_tensor, kv_index, 1, keepdims=False)
            value_head = lax.dynamic_index_in_dim(value_tensor, kv_index, 1, keepdims=False)
            scores = jnp.dot(query_head, key_head.T, preferred_element_type=jnp.float32) * scale
            scores = jnp.where(causal, scores, jnp.float32(-1e+30))
            top = lax.optimization_barrier(jnp.max(scores, axis=-1, keepdims=True))
            weights = jnp.exp(scores - top)
            probs = (weights / lax.optimization_barrier(jnp.sum(weights, axis=-1, keepdims=True))).astype(jnp.bfloat16)
            return jnp.dot(probs, value_head, preferred_element_type=jnp.float32).astype(jnp.bfloat16)
        heads = lax.map(one_head, jnp.arange(HQ, dtype=jnp.int32))
        heads = jnp.transpose(heads, (1, 0, 2)).reshape(SEQUENCE_TOKENS, HQ * HEAD_SIZE)
        branch = jnp.dot(heads, w_out, preferred_element_type=jnp.float32).astype(jnp.bfloat16)
        return sequence_rows.astype(jnp.float32) + branch.astype(jnp.float32)
    return lax.map(one_sequence, tokens)
```

```python
import functools

import jax
import jax.numpy as jnp
from jax import lax
from jax.experimental import pallas as pl
from jax.experimental.pallas import tpu as pltpu
from jax.sharding import Mesh
from jax.sharding import PartitionSpec as P

HEAD_SIZE = 128
F32 = jnp.float32
BF16 = jnp.bfloat16
SMEM = pl.BlockSpec(memory_space=pltpu.SMEM)
VMEM = pl.BlockSpec(memory_space=pltpu.VMEM)


class Grid:
    def __init__(self, ny, nx, nz, nc):
        self.ny, self.nx, self.nz, self.nc = ny, nx, nz, nc
        self.nb = ny * nx

    def place(self, me):
        c = lax.rem(me, self.nc)
        z = lax.rem(me // self.nc, self.nz)
        b = me // (self.nc * self.nz)
        return b // self.nx, lax.rem(b, self.nx), z, c

    def blocks(self, y, x):
        return [
            lax.rem(y + dy, self.ny) * self.nx + lax.rem(x + dx, self.nx)
            for dy in range(self.ny)
            for dx in range(self.nx)
        ]


def shift(value, axis, size, step):
    return lax.ppermute(value, axis, [((i + step) % size, i) for i in range(size)])


def norm_kernel(grid, rows, me_ref, x_ref, gain_ref, *outs):
    y, x, z, c = grid.place(me_ref[0])
    floats = x_ref[...].astype(F32)
    mean_square = jnp.mean(floats * floats, axis=-1, keepdims=True)
    factor = lax.rsqrt(mean_square + 1e-05)
    width = grid.nc * rows
    for dz in range(grid.nz):
        zz = lax.rem(z + dz, grid.nz)
        for i, block in enumerate(grid.blocks(y, x)):
            at = pl.multiple_of((block * grid.nz + zz) * width, width)
            piece = x_ref[:, pl.ds(at, width)].astype(F32) * factor * gain_ref[:, pl.ds(at, width)]
            swapped = jnp.concatenate([piece[:, rows:], piece[:, :rows]], axis=1)
            outs[dz][:, i * width : (i + 1) * width] = jnp.where(c == 0, piece, swapped).astype(BF16)


def norm(grid, me, tokens, gain, rows):
    count, width = tokens.shape
    step = 32
    part = width // grid.nz
    return pl.pallas_call(
        functools.partial(norm_kernel, grid, rows),
        grid=(count // step,),
        in_specs=[
            SMEM,
            pl.BlockSpec((step, width), lambda i: (i, 0)),
            pl.BlockSpec((1, width), lambda i: (0, 0)),
        ],
        out_specs=[pl.BlockSpec((step, part), lambda i: (i, 0))] * grid.nz,
        out_shape=[jax.ShapeDtypeStruct((count, part), BF16)] * grid.nz,
        cost_estimate=pl.CostEstimate(flops=count * width * 8, bytes_accessed=count * width * 4, transcendentals=0),
        name="norm",
    )(me, tokens, gain)


def project_kernel(count, x_ref, *refs):
    weights, outs = refs[:count], refs[count:]
    depth = weights[0].shape[0]
    total = None
    for i, w_ref in enumerate(weights):
        term = jnp.dot(x_ref[:, i * depth : (i + 1) * depth], w_ref[...], preferred_element_type=F32)
        total = term if total is None else total + term
    tall = outs[0].shape[0]
    for i, out in enumerate(outs):
        out[...] = total[i * tall : (i + 1) * tall].astype(BF16)


def project(grid, x, weights):
    tall, deep = x.shape
    depth, width = weights[0].shape
    tile = min(width, 256)
    part = tall // grid.nz
    return pl.pallas_call(
        functools.partial(project_kernel, len(weights)),
        grid=(width // tile,),
        in_specs=[pl.BlockSpec((tall, deep), lambda i: (0, 0))]
        + [pl.BlockSpec((depth, tile), lambda i: (0, i))] * len(weights),
        out_specs=[pl.BlockSpec((part, tile), lambda i: (0, i))] * grid.nz,
        out_shape=[jax.ShapeDtypeStruct((part, width), BF16)] * grid.nz,
        cost_estimate=pl.CostEstimate(
            flops=2 * tall * deep * width, bytes_accessed=2 * (tall * deep + deep * width + tall * width), transcendentals=0
        ),
        name="project",
    )(x, *weights)


def combine_kernel(grid, me_ref, a_ref, b_ref, c_ref, *outs):
    y, x, _, _ = grid.place(me_ref[0])
    width = outs[0].shape[1]
    for out, block in zip(outs, grid.blocks(y, x)):
        at = pl.ds(pl.multiple_of(block * width, width), width)
        out[...] = (a_ref[:, at].astype(F32) + b_ref[:, at].astype(F32) + c_ref[:, at].astype(F32)).astype(BF16)


def combine(grid, me, own, up, down):
    tall, width = own.shape
    return pl.pallas_call(
        functools.partial(combine_kernel, grid),
        in_specs=[SMEM, VMEM, VMEM, VMEM],
        out_specs=[VMEM] * grid.nb,
        out_shape=[jax.ShapeDtypeStruct((tall, width // grid.nb), BF16)] * grid.nb,
        cost_estimate=pl.CostEstimate(flops=tall * width * 2, bytes_accessed=tall * width * 8, transcendentals=0),
        name="combine",
    )(me, own, up, down)


def attend_kernel(grid, heads, me_ref, *refs):
    nb = grid.nb
    pairs, queries = refs[:nb], refs[nb : 2 * nb]
    out, keys, values, all_queries = refs[2 * nb :]
    y, x, _, _ = grid.place(me_ref[0])
    part = pairs[0].shape[0]
    for pair, query, block in zip(pairs, queries, grid.blocks(y, x)):
        at = pl.ds(pl.multiple_of(block * part, part), part)
        keys[at, :] = pair[:, :HEAD_SIZE]
        values[at, :] = pair[:, HEAD_SIZE:]
        all_queries[at, :] = query[...]
    length = keys.shape[0]
    step = min(length, 256)
    scale = HEAD_SIZE ** (-0.5)
    for head in range(heads):
        cols = slice(head * HEAD_SIZE, (head + 1) * HEAD_SIZE)
        for first in range(0, length, step):
            seen = first + step
            scores = (
                lax.dot_general(
                    all_queries[first:seen, cols],
                    keys[:seen, :],
                    (((1,), (1,)), ((), ())),
                    preferred_element_type=F32,
                )
                * scale
            )
            row = lax.broadcasted_iota(jnp.int32, (step, seen), 0) + first
            col = lax.broadcasted_iota(jnp.int32, (step, seen), 1)
            scores = jnp.where(row >= col, scores, F32(-1e30))
            top = jnp.max(scores, axis=-1, keepdims=True)
            weights = jnp.exp(scores - top)
            probs = (weights * (1.0 / jnp.sum(weights, axis=-1, keepdims=True))).astype(BF16)
            out[first:seen, cols] = jnp.dot(probs, values[:seen, :], preferred_element_type=F32).astype(BF16)


def attend(grid, me, pairs, queries):
    part, width = queries[0].shape
    heads = width // HEAD_SIZE
    length = part * grid.nb
    return pl.pallas_call(
        functools.partial(attend_kernel, grid, heads),
        in_specs=[SMEM] + [VMEM] * (2 * grid.nb),
        out_specs=VMEM,
        out_shape=jax.ShapeDtypeStruct((length, width), BF16),
        scratch_shapes=[
            pltpu.VMEM((length, HEAD_SIZE), BF16),
            pltpu.VMEM((length, HEAD_SIZE), BF16),
            pltpu.VMEM((length, width), BF16),
        ],
        cost_estimate=pl.CostEstimate(
            flops=heads * length * length * HEAD_SIZE * 8, bytes_accessed=length * width * 4, transcendentals=heads * length * length
        ),
        name="attend",
    )(me, *pairs, *queries)


def mix_kernel(grid, firsts, local_heads, shards, me_ref, *refs):
    nb = grid.nb
    pieces = refs[: len(firsts) * nb]
    weights = refs[len(firsts) * nb : len(firsts) * nb + shards]
    outs = refs[len(firsts) * nb + shards : -1]
    total = refs[-1]
    y, x, _, _ = grid.place(me_ref[0])
    blocks = grid.blocks(y, x)
    run = None
    for j, head in enumerate(firsts):
        for i, block in enumerate(blocks):
            piece = pieces[j * nb + i]
            deep = piece.shape[1]
            at = pl.ds(pl.multiple_of((block * local_heads + head) * HEAD_SIZE, HEAD_SIZE), deep)
            w = jnp.concatenate([w_ref[at, :] for w_ref in weights], axis=1)
            term = jnp.dot(piece[...], w, preferred_element_type=F32)
            run = term if run is None else run + term
    total[...] = run
    part = outs[0].shape[0]
    for out, block in zip(outs, blocks):
        out[...] = total[pl.ds(pl.multiple_of(block * part, part), part), :].astype(BF16)


def mix(grid, me, groups, firsts, local_heads, weights):
    pieces = [piece for group in groups for piece in group]
    length = pieces[0].shape[0]
    deep = weights[0].shape[0]
    width = sum(w.shape[1] for w in weights)
    part = length // grid.nb
    return pl.pallas_call(
        functools.partial(mix_kernel, grid, firsts, local_heads, len(weights)),
        in_specs=[SMEM] + [VMEM] * (len(pieces) + len(weights)),
        out_specs=[VMEM] * grid.nb,
        out_shape=[jax.ShapeDtypeStruct((part, width), BF16)] * grid.nb,
        scratch_shapes=[pltpu.VMEM((length, width), F32)],
        cost_estimate=pl.CostEstimate(
            flops=2 * length * deep * width, bytes_accessed=2 * (length * deep + deep * width), transcendentals=0
        ),
        name="mix",
    )(me, *pieces, *weights)


def finish_kernel(grid, me_ref, x_ref, *refs):
    pieces, out = refs[:-1], refs[-1]
    y, x, z, c = grid.place(me_ref[0])
    width = pieces[0].shape[1]
    half = width // grid.nc
    for dz in range(grid.nz):
        zz = lax.rem(z + dz, grid.nz)
        for i, block in enumerate(grid.blocks(y, x)):
            piece = pieces[dz * grid.nb + i][...].astype(F32)
            swapped = jnp.concatenate([piece[:, half:], piece[:, :half]], axis=1)
            at = pl.ds(pl.multiple_of((block * grid.nz + zz) * width, width), width)
            out[:, at] = x_ref[:, at].astype(F32) + jnp.where(c == 0, piece, swapped)


def finish(grid, me, tokens, pieces):
    count, width = tokens.shape
    step = 32
    return pl.pallas_call(
        functools.partial(finish_kernel, grid),
        grid=(count // step,),
        in_specs=[SMEM, pl.BlockSpec((step, width), lambda i: (i, 0))]
        + [pl.BlockSpec((step, piece.shape[1]), lambda i: (i, 0)) for piece in pieces],
        out_specs=pl.BlockSpec((step, width), lambda i: (i, 0)),
        out_shape=jax.ShapeDtypeStruct((count, width), F32),
        cost_estimate=pl.CostEstimate(flops=count * width, bytes_accessed=count * width * 8, transcendentals=0),
        name="finish",
    )(me, tokens, *pieces)


def spread(grid, value, x_first):
    if x_first:
        near = [value] + [shift(value, "x", grid.nx, d) for d in range(1, grid.nx)]
        far = [near] + [[shift(v, "y", grid.ny, d) for v in near] for d in range(1, grid.ny)]
        return [v for line in far for v in line]
    near = [value] + [shift(value, "y", grid.ny, d) for d in range(1, grid.ny)]
    far = [near] + [[shift(v, "x", grid.nx, d) for v in near] for d in range(1, grid.nx)]
    return [far[dx][dy] for dy in range(grid.ny) for dx in range(grid.nx)]


def exchange(grid, pieces):
    out = [pieces[0]]
    n, ny, nx = grid.nb, grid.ny, grid.nx
    for i in range(1, n):
        dy, dx = i // nx, i % nx
        back_y, back_x = (-dy) % ny, (-dx) % nx
        pairs = []
        for y in range(ny):
            for x in range(nx):
                pairs.append((((y + dy) % ny) * nx + (x + dx) % nx, y * nx + x))
        out.append(lax.ppermute(pieces[back_y * nx + back_x], ("y", "x"), pairs))
    return out


def reduce_line(grid, parts):
    n = grid.nz
    up = down = None
    for s in range(1, n):
        send_up = parts[n - s]
        send_down = parts[s]
        if up is not None:
            send_up = (send_up.astype(F32) + up.astype(F32)).astype(BF16)
            send_down = (send_down.astype(F32) + down.astype(F32)).astype(BF16)
        up = lax.ppermute(send_up, "z", [(i, i + 1) for i in range(s)])
        down = lax.ppermute(send_down, "z", [(n - 1 - i, n - 2 - i) for i in range(s)])
    return parts[0], up, down


def gather_line(grid, value):
    n = grid.nz
    ups, downs = [], []
    up = down = value
    for s in range(1, n):
        up = lax.ppermute(up, "z", [(i, i + 1) for i in range(s - 1, n - 1)])
        down = lax.ppermute(down, "z", [(i, i - 1) for i in range(1, n - s + 1)])
        ups.append(up)
        downs.append(down)
    z = lax.axis_index("z")
    return [value] + [jnp.where(z + d < n, downs[d - 1], ups[n - d - 1]) for d in range(1, n)]


def head_runs(local_heads):
    step = 2 if local_heads % 2 == 0 else 1
    return [(first, step) for first in range(0, local_heads, step)]


def body(grid, tokens, norm_gain, w_query, key_weight, value_weight, w_out):
    me = lax.axis_index(("y", "x", "z", "c")).reshape(1)
    nb, nz, nc = grid.nb, grid.nz, grid.nc
    rows = w_query.shape[0]
    query_heads = w_query.shape[1] // HEAD_SIZE
    key_heads = key_weight.shape[1] // HEAD_SIZE
    local_heads = query_heads // nb
    group = query_heads // key_heads

    kinds = []
    for b in range(nb):
        at = b * local_heads // group * HEAD_SIZE
        kinds += [key_weight[:, at : at + HEAD_SIZE], value_weight[:, at : at + HEAD_SIZE]]
    chunks = [jnp.concatenate(kinds, axis=1)]
    runs = head_runs(local_heads)
    by_head = w_query.reshape(rows, nb, local_heads * HEAD_SIZE)
    for first, count in runs:
        piece = by_head[:, :, first * HEAD_SIZE : (first + count) * HEAD_SIZE]
        chunks.append(piece.reshape(rows, nb * count * HEAD_SIZE))

    x0 = tokens[0]
    normed = norm(grid, me, x0, norm_gain.reshape(1, -1), rows)
    arrived = [normed[0]] + [
        lax.ppermute(normed[(-d) % nz], "z", [((i + d) % nz, i) for i in range(nz)]) for d in range(1, nz)
    ]
    x = jnp.concatenate(arrived, axis=0)

    reduced = []
    for j, chunk in enumerate(chunks):
        held = spread(grid, chunk, j % 2 == 1)
        weights = []
        for w in held:
            weights += [w] + [shift(w, "c", nc, d) for d in range(1, nc)]
        parts = project(grid, x, weights)
        own, up, down = reduce_line(grid, parts)
        reduced.append(exchange(grid, combine(grid, me, own, up, down)))

    columns = w_out.shape[1]
    cuts = 2 if columns % 256 == 0 else 1
    width = columns // cuts
    lines = [gather_line(grid, w_out[:, i * width : (i + 1) * width]) for i in range(cuts)]

    groups = []
    for j in range(len(runs)):
        attended = attend(grid, me, reduced[0], reduced[j + 1])
        groups.append(spread(grid, attended, j % 2 == 0))

    pieces = []
    for dz in range(nz):
        own = [line[dz] for line in lines]
        weights = own + [shift(w, "c", nc, d) for d in range(1, nc) for w in own]
        mixed = mix(grid, me, groups, [first for first, _ in runs], local_heads, weights)
        pieces += exchange(grid, mixed)
    return finish(grid, me, x0, pieces)[None]


def solution(mesh):
    seq, fsdp = mesh.shape["seq"], mesh.shape["fsdp"]
    nx = 2 if seq % 2 == 0 else 1
    nc = 2
    grid = Grid(seq // nx, nx, fsdp // nc, nc)
    fine = Mesh(mesh.devices.reshape(grid.ny, grid.nx, grid.nz, grid.nc), ("y", "x", "z", "c"))
    everywhere = ("y", "x", "z", "c")
    placed = (
        P(("z", "c"), ("y", "x"), None),
        P(),
        P(everywhere, None),
        P(everywhere, None),
        P(everywhere, None),
        P(None, everywhere),
    )
    return jax.shard_map(
        functools.partial(body, grid),
        mesh=fine,
        in_specs=placed,
        out_specs=P(("z", "c"), ("y", "x"), None),
        check_vma=False,
    )
```
